32 devices in a mesh: farcp: 2 (over x), nearcp: 4 (over y, core), model: 4 (over z).
Axes of the slice: x: 2, y: 2, z: 4, core: 2. Of those that a mesh axis runs over, the one named last changes fastest.
Arguments:
- raw_keys: bfloat16 [8, 8192, 8, 128], P(None, ('farcp', 'nearcp'), 'model'), may hold values from -6 to 6
- raw_values: bfloat16 [8, 8192, 8, 128], P(None, ('farcp', 'nearcp'), 'model'), may hold values from -6 to 6
- turn_angle: float32 [8192, 64], replicated, may hold values from -3.140625 to 3.140625
- key_gain: float32 [128], replicated, may hold values from 0.25 to 1.75
Outputs:
- stored_keys: bfloat16 [8, 8192, 8, 128], P(('farcp', 'nearcp'), None, 'model')
- stored_values: bfloat16 [8, 8192, 8, 128], P(('farcp', 'nearcp'), None, 'model')
- key_scale: float32 [8, 8, 128], P(('farcp', 'nearcp'), 'model')
The draws below stay inside these ranges and needn't reach their ends.
All inputs are finite; a program needn't handle non-finite values. Where the reference program divides by a largest or mean magnitude, that divisor is 1e-20 or more.
Results may differ from the reference program's by a relative error of at most 0.001.
Values may be sent and summed in bfloat16 or wider, within the bound.
No kernel may reach another device: no remote copies, remote signals or barrier semaphores. Data moves between devices by JAX's collectives and lax.ppermute only.
A program may use at most 192 MiB of HBM per device.

```python
import jax
import jax.numpy as jnp
from jax import lax

BATCH = 8
LENGTH = 8192
KV_HEADS = 8
HEAD_SIZE = 128
HALF_HEAD = 64


def steps_of(rng, extent, cuts, low, largest):
    loudness = 1.0
    for dim, shards_of in cuts:
        draws = jax.random.uniform(jax.random.fold_in(jax.random.fold_in(rng, 6), dim), (shards_of,), jnp.float32, low / len(cuts), largest / len(cuts))
        loudness = loudness * jnp.repeat(jnp.exp(draws), extent[dim] // shards_of).reshape((-1,) + (1,) * (len(extent) - 1 - dim))
    return loudness


def gaussian(stream_key, extent, scale, reach, pieces=(), dtype=jnp.bfloat16):
    array = scale * jax.random.normal(stream_key, extent, jnp.float32)
    if pieces:
        array = array * steps_of(stream_key, extent, pieces, -0.22, 0.18)
    return jnp.clip(array, -reach, reach).astype(dtype)


def setup_inputs(seed: int = 0) -> dict:
    keys = jax.random.split(jax.random.key(seed), 5)
    return {
        "raw_keys": gaussian(keys[0], (BATCH, LENGTH, KV_HEADS, HEAD_SIZE), 1.0, 6.0, ((1, 8), (2, 4))),
        "raw_values": gaussian(keys[1], (BATCH, LENGTH, KV_HEADS, HEAD_SIZE), 1.0, 6.0, ((1, 8), (2, 4))),
        "turn_angle": jnp.clip(jax.random.uniform(keys[2], (LENGTH, HALF_HEAD), jnp.float32, -3.140625, 3.140625), -3.140625, 3.140625),
        "key_gain": jnp.clip(1.0 + 0.15 * jax.random.normal(keys[3], (HEAD_SIZE,), jnp.float32), 0.25, 1.75),
    }


def apply_rotary(vectors, angle):
    half = vectors.shape[-1] // 2
    cosine, sine = (jnp.cos(angle)[None, :, None, :], jnp.sin(angle)[None, :, None, :])
    first, second = (vectors[..., :half], vectors[..., half:])
    return jnp.concatenate([first * cosine - second * sine, second * cosine + first * sine], axis=-1)

def scale_rows(vectors, row_gain):
    return vectors * lax.rsqrt(lax.optimization_barrier(jnp.mean(vectors * vectors, axis=-1, keepdims=True)) + 1e-06) * row_gain

def prepare_keys(plain_keys, angle, key_gain):
    wide_keys = plain_keys.astype(jnp.float32)
    wide_keys = scale_rows(wide_keys, key_gain)
    return apply_rotary(wide_keys, angle)

def reference(raw_keys, raw_values, turn_angle, key_gain):
    turned_keys = prepare_keys(raw_keys, turn_angle, key_gain)
    key_scale = lax.optimization_barrier(jnp.max(jnp.abs(turned_keys), axis=1))
    narrow_keys = (turned_keys / key_scale[:, None]).astype(jnp.bfloat16)
    stored_keys = narrow_keys
    stored_values = raw_values
    return (stored_keys, stored_values, key_scale)
```

```python
import functools
import math

import jax
import jax.numpy as jnp
from jax import lax
from jax.experimental import pallas as pl
from jax.experimental.pallas import tpu as pltpu
from jax.sharding import PartitionSpec as P

GROUP = ("farcp", "nearcp")
TILE = 128


def partner(me, step, count):
    if count & (count - 1) == 0:
        return me ^ step
    return lax.rem(me + step, count)


def sender(me, step, count):
    if count & (count - 1) == 0:
        return me ^ step
    return lax.rem(me + count - step, count)


def in_hbm(array):
    return pltpu.with_memory_space_constraint(array, pltpu.HBM)


def cut_kernel(count, steps, whole, *refs):
    pieces, sems = refs[: len(steps)], refs[len(steps)]
    me = lax.axis_index(GROUP)
    copies = [
        pltpu.make_async_copy(whole.at[partner(me, step, count)], piece, sems.at[slot])
        for slot, (step, piece) in enumerate(zip(steps, pieces))
    ]
    for copy in copies:
        copy.start()
    for copy in copies:
        copy.wait()


def cut(whole, steps):
    count, rows, lanes = whole.shape
    return pl.pallas_call(
        functools.partial(cut_kernel, count, steps),
        out_shape=[pltpu.VMEM((rows, lanes), whole.dtype)] * len(steps),
        in_specs=[pl.BlockSpec(memory_space=pltpu.HBM)],
        out_specs=[pl.BlockSpec(memory_space=pltpu.VMEM)] * len(steps),
        scratch_shapes=[pltpu.SemaphoreType.DMA((len(steps),))],
        compiler_params=pltpu.CompilerParams(vmem_limit_bytes=8 << 20),
    )(in_hbm(whole))


def exchange(pieces, steps, count):
    return [
        lax.ppermute(
            piece, GROUP, [(source, source ^ step if count & (count - 1) == 0 else (source + step) % count) for source in range(count)]
        )
        for step, piece in zip(steps, pieces)
    ]


def keys_kernel(count, heads, steps, own, *refs):
    number = len(steps)
    pieces = refs[:number]
    cosine, sine, gain, stored, scale = refs[number : number + 5]
    block, turned, cos_in, sin_in, cos_rows, sin_rows, out, in_sems, tab_sems, out_sems = refs[number + 5 :]
    rows, lanes = block.shape
    length = rows // heads
    half = lanes // 2
    me = lax.axis_index(GROUP)
    sources = [me] + [sender(me, step, count) for step in steps]
    first = pltpu.make_async_copy(own.at[me], block, in_sems)
    first.start()

    def tables(slot):
        start = sources[slot] * length
        return (
            pltpu.make_async_copy(cosine.at[pl.ds(start, length)], cos_in.at[slot % 2], tab_sems.at[slot % 2, 0]),
            pltpu.make_async_copy(sine.at[pl.ds(start, length)], sin_in.at[slot % 2], tab_sems.at[slot % 2, 1]),
        )

    for copy in tables(0):
        copy.start()
    first.wait()
    peak = jnp.zeros((8, lanes), jnp.float32)
    factor = gain[...]
    for slot in range(number + 1):
        piece = block if slot == 0 else pieces[slot - 1]
        for copy in tables(slot):
            copy.wait()
        if slot < number:
            for copy in tables(slot + 1):
                copy.start()

        def spread(index, carry, slot=slot):
            part = pl.ds(pl.multiple_of(index * 64, 64), 64)
            c = cos_in[slot % 2, part, :]
            s = sin_in[slot % 2, part, :]
            for head in range(heads):
                at = pl.ds(index * 64 * heads + head, 64, stride=heads)
                cos_rows[at, :] = jnp.concatenate([c, c], axis=-1)
                sin_rows[at, :] = jnp.concatenate([-s, s], axis=-1)
            return carry

        lax.fori_loop(0, length // 64, spread, 0)

        def turn(index, peak, slot=slot, piece=piece):
            part = pl.ds(pl.multiple_of(index * TILE, TILE), TILE)
            wide = piece[part, :].astype(jnp.float32)
            mean = jnp.sum(wide * wide, axis=-1, keepdims=True) * (1.0 / lanes)
            wide = wide * lax.rsqrt(mean + 1e-06) * factor
            wide = wide * cos_rows[part, :] + pltpu.roll(wide, half, 1) * sin_rows[part, :]
            turned[slot, part, :] = wide
            return jnp.maximum(peak, jnp.max(jnp.abs(wide).reshape(TILE // 8, 8, lanes), axis=0))

        peak = lax.fori_loop(0, rows // TILE, turn, peak)
    tops = [peak[head : head + 1] for head in range(heads)]
    for row in range(heads, 8):
        tops[row % heads] = jnp.maximum(tops[row % heads], peak[row : row + 1])
    top = jnp.concatenate(tops, axis=0)
    scale[...] = top
    inverse = 1.0 / jnp.concatenate([top] * (8 // heads), axis=0)
    for slot in range(number + 1):
        copy = pltpu.make_async_copy(
            out.at[slot % 2], stored.at[pl.ds(sources[slot] * rows, rows)], out_sems.at[slot % 2]
        )
        if slot >= 2:
            copy.wait()

        def narrow(index, carry, slot=slot):
            part = pl.ds(pl.multiple_of(index * TILE, TILE), TILE)
            wide = turned[slot, part, :].reshape(TILE // 8, 8, lanes) * inverse[None]
            out[slot % 2, part, :] = wide.reshape(TILE, lanes).astype(out.dtype)
            return carry

        lax.fori_loop(0, rows // TILE, narrow, 0)
        copy.start()
    for slot in range(max(number - 1, 0), number + 1):
        pltpu.make_async_copy(
            out.at[slot % 2], stored.at[pl.ds(sources[slot] * rows, rows)], out_sems.at[slot % 2]
        ).wait()


def finish_keys(own, pieces, cosine, sine, gain, steps, heads):
    count, rows, lanes = own.shape
    length = rows // heads
    return pl.pallas_call(
        functools.partial(keys_kernel, count, heads, steps),
        out_shape=[
            jax.ShapeDtypeStruct((count * rows, lanes), own.dtype),
            jax.ShapeDtypeStruct((heads, lanes), jnp.float32),
        ],
        in_specs=[pl.BlockSpec(memory_space=pltpu.HBM)]
        + [pl.BlockSpec(memory_space=pltpu.VMEM)] * len(pieces)
        + [pl.BlockSpec(memory_space=pltpu.HBM)] * 2
        + [pl.BlockSpec(memory_space=pltpu.VMEM)],
        out_specs=[pl.BlockSpec(memory_space=pltpu.HBM), pl.BlockSpec(memory_space=pltpu.VMEM)],
        scratch_shapes=[
            pltpu.VMEM((rows, lanes), own.dtype),
            pltpu.VMEM((count, rows, lanes), jnp.float32),
            pltpu.VMEM((2, length, lanes // 2), jnp.float32),
            pltpu.VMEM((2, length, lanes // 2), jnp.float32),
            pltpu.VMEM((rows, lanes), jnp.float32),
            pltpu.VMEM((rows, lanes), jnp.float32),
            pltpu.VMEM((2, rows, lanes), own.dtype),
            pltpu.SemaphoreType.DMA,
            pltpu.SemaphoreType.DMA((2, 2)),
            pltpu.SemaphoreType.DMA((2,)),
        ],
        compiler_params=pltpu.CompilerParams(vmem_limit_bytes=32 << 20),
        cost_estimate=pl.CostEstimate(flops=count * rows * lanes * 200, bytes_accessed=count * rows * lanes * 8, transcendentals=0),
    )(in_hbm(own), *pieces, in_hbm(cosine), in_hbm(sine), gain)


def place_kernel(count, steps, after, own, *refs):
    del after
    number = len(steps)
    pieces = refs[:number]
    whole, block, in_sem, sems = refs[number : number + 4]
    rows, lanes = block.shape
    me = lax.axis_index(GROUP)
    first = pltpu.make_async_copy(own.at[me], block, in_sem)
    first.start()
    copies = [
        pltpu.make_async_copy(piece, whole.at[pl.ds(sender(me, step, count) * rows, rows)], sems.at[slot])
        for slot, (step, piece) in enumerate(zip(steps, pieces))
    ]
    for copy in copies:
        copy.start()
    first.wait()
    last = pltpu.make_async_copy(block, whole.at[pl.ds(me * rows, rows)], in_sem)
    last.start()
    for copy in copies:
        copy.wait()
    last.wait()


def place(after, own, pieces, steps):
    count, rows, lanes = own.shape
    return pl.pallas_call(
        functools.partial(place_kernel, count, steps),
        out_shape=jax.ShapeDtypeStruct((count * rows, lanes), own.dtype),
        in_specs=[pl.BlockSpec(memory_space=pltpu.HBM)] * 2 + [pl.BlockSpec(memory_space=pltpu.VMEM)] * len(pieces),
        out_specs=pl.BlockSpec(memory_space=pltpu.HBM),
        scratch_shapes=[
            pltpu.VMEM((rows, lanes), own.dtype),
            pltpu.SemaphoreType.DMA,
            pltpu.SemaphoreType.DMA((len(steps),)),
        ],
        compiler_params=pltpu.CompilerParams(vmem_limit_bytes=8 << 20),
    )(in_hbm(after), in_hbm(own), *pieces)


def local(raw_keys, raw_values, turn_angle, key_gain):
    count, length, heads, lanes = raw_keys.shape
    rows = length * heads
    keys = raw_keys.reshape(count, rows, lanes)
    values = raw_values.reshape(count, rows, lanes)
    steps = tuple(sorted(range(1, count), key=lambda step: (-bin(step // 2).count("1"), step)))
    key_pieces = exchange(cut(keys, steps), steps, count)
    value_pieces = exchange(cut(values, steps), steps, count)
    cosine, sine = jnp.cos(turn_angle), jnp.sin(turn_angle)
    stored_keys, key_scale = finish_keys(keys, key_pieces, cosine, sine, key_gain.reshape(1, lanes), steps, heads)
    stored_values = place(key_scale, values, value_pieces, steps)
    whole = (1, count * length, heads, lanes)
    return stored_keys.reshape(whole), stored_values.reshape(whole), key_scale[None]


def solution(mesh):
    in_specs = (
        P(None, GROUP, "model", None),
        P(None, GROUP, "model", None),
        P(),
        P(),
    )
    out_specs = (
        P(GROUP, None, "model", None),
        P(GROUP, None, "model", None),
        P(GROUP, "model", None),
    )
    return jax.shard_map(local, mesh=mesh, in_specs=in_specs, out_specs=out_specs, check_vma=False)
```

```python
import functools

import jax
import jax.numpy as jnp
from jax import lax
from jax.experimental import pallas as pl
from jax.experimental.pallas import tpu as pltpu
from jax.sharding import PartitionSpec as P


GROUP = ("farcp", "nearcp")
TILE = 128
UNROLL = 2


def partner(me, step, count):
    return me ^ step if count & (count - 1) == 0 else (me + step) % count


def sender(me, step, count):
    return me ^ step if count & (count - 1) == 0 else (me + count - step) % count


def orders(count):
    def hops(step):
        return bin(step >> 1).count("1")

    steps = range(1, count)
    keys = sorted(steps, key=lambda step: (step < 2, step & 1, -hops(step), step))
    values = sorted(steps, key=lambda step: (hops(step), step & 1, -step))
    return tuple(keys), tuple(values)


def in_hbm(array):
    return pltpu.with_memory_space_constraint(array, pltpu.HBM)


def cut_kernel(count, steps, whole, *refs):
    pieces, sems = refs[: len(steps)], refs[len(steps)]
    me = lax.axis_index(GROUP)
    copies = [
        pltpu.make_async_copy(whole.at[partner(me, step, count)], piece, sems.at[slot])
        for slot, (step, piece) in enumerate(zip(steps, pieces))
    ]
    for copy in copies:
        copy.start()
    for copy in copies:
        copy.wait()


def cut(whole, steps):
    count, rows, lanes = whole.shape
    return pl.pallas_call(
        functools.partial(cut_kernel, count, steps),
        out_shape=[pltpu.VMEM((rows, lanes), whole.dtype)] * len(steps),
        in_specs=[pl.BlockSpec(memory_space=pltpu.HBM)],
        out_specs=[pl.BlockSpec(memory_space=pltpu.VMEM)] * len(steps),
        scratch_shapes=[pltpu.SemaphoreType.DMA((len(steps),))],
        compiler_params=pltpu.CompilerParams(vmem_limit_bytes=8 << 20),
    )(in_hbm(whole))


def exchange(pieces, steps, count):
    moved = []
    for step, piece in zip(steps, pieces):
        pairs = [(source, int(partner(source, step, count))) for source in range(count)]
        moved.append(lax.ppermute(piece, GROUP, pairs))
    return moved


def table_kernel(heads, angle, cosine, sine):
    turn = angle[...]
    c, s = jnp.cos(turn), jnp.sin(turn)
    c = jnp.concatenate([c, c], axis=0).T
    s = jnp.concatenate([-s, s], axis=0).T
    for head in range(heads):
        at = pl.ds(head, c.shape[0], stride=heads)
        cosine[at, :] = c
        sine[at, :] = s


def tables(turn_angle, heads, block=512):
    length, half = turn_angle.shape
    shape = pltpu.HBM((length * heads, 2 * half), jnp.float32)
    return pl.pallas_call(
        functools.partial(table_kernel, heads),
        out_shape=[shape, shape],
        grid=(length // block,),
        in_specs=[pl.BlockSpec((half, block), lambda i: (0, i))],
        out_specs=[pl.BlockSpec((block * heads, 2 * half), lambda i: (i, 0))] * 2,
        compiler_params=pltpu.CompilerParams(vmem_limit_bytes=8 << 20),
        cost_estimate=pl.CostEstimate(flops=length * half * 400, bytes_accessed=length * half * 40, transcendentals=0),
    )(in_hbm(turn_angle.T))


def keys_kernel(count, heads, steps, own, *refs):
    number = len(steps)
    pieces = refs[:number]
    cosine, sine, gain, stored, scale = refs[number : number + 5]
    block, turned, cos_in, sin_in, out, in_sems, tab_sems, out_sems = refs[number + 5 :]
    rows, lanes = block.shape
    half = lanes // 2
    me = lax.axis_index(GROUP)
    sources = [me] + [sender(me, step, count) for step in steps]
    first = pltpu.make_async_copy(own.at[me], block, in_sems)
    first.start()

    def fetch(slot):
        part = pl.ds(sources[slot] * rows, rows)
        return (
            pltpu.make_async_copy(cosine.at[part], cos_in.at[slot % 2], tab_sems.at[slot % 2, 0]),
            pltpu.make_async_copy(sine.at[part], sin_in.at[slot % 2], tab_sems.at[slot % 2, 1]),
        )

    for copy in fetch(0):
        copy.start()
    first.wait()
    peak = jnp.zeros((8, lanes), jnp.float32)
    factor = gain[...]
    for slot in range(number + 1):
        piece = block if slot == 0 else pieces[slot - 1]
        for copy in fetch(slot):
            copy.wait()
        if slot < number:
            for copy in fetch(slot + 1):
                copy.start()

        def turn(index, peak, slot=slot, piece=piece):
            part = pl.ds(pl.multiple_of(index * TILE, TILE), TILE)
            wide = piece[part, :].astype(jnp.float32)
            mean = jnp.sum(wide * wide, axis=-1, keepdims=True) * (1.0 / lanes)
            wide = wide * lax.rsqrt(mean + 1e-06) * factor
            wide = wide * cos_in[slot % 2, part, :] + pltpu.roll(wide, half, 1) * sin_in[slot % 2, part, :]
            turned[slot, part, :] = wide
            return jnp.maximum(peak, jnp.max(jnp.abs(wide).reshape(TILE // 8, 8, lanes), axis=0))

        peak = lax.fori_loop(0, rows // TILE, turn, peak, unroll=UNROLL)
    tops = [peak[head : head + 1] for head in range(heads)]
    for row in range(heads, 8):
        tops[row % heads] = jnp.maximum(tops[row % heads], peak[row : row + 1])
    top = jnp.concatenate(tops, axis=0)
    scale[...] = top
    inverse = 1.0 / jnp.concatenate([top] * (8 // heads), axis=0)
    for slot in range(number + 1):
        copy = pltpu.make_async_copy(
            out.at[slot % 2], stored.at[pl.ds(sources[slot] * rows, rows)], out_sems.at[slot % 2]
        )
        if slot >= 2:
            copy.wait()

        def narrow(index, carry, slot=slot):
            part = pl.ds(pl.multiple_of(index * TILE, TILE), TILE)
            wide = turned[slot, part, :].reshape(TILE // 8, 8, lanes) * inverse[None]
            out[slot % 2, part, :] = wide.reshape(TILE, lanes).astype(out.dtype)
            return carry

        lax.fori_loop(0, rows // TILE, narrow, 0, unroll=UNROLL)
        copy.start()
    for slot in range(max(number - 1, 0), number + 1):
        pltpu.make_async_copy(
            out.at[slot % 2], stored.at[pl.ds(sources[slot] * rows, rows)], out_sems.at[slot % 2]
        ).wait()


def finish_keys(own, pieces, cosine, sine, gain, steps, heads):
    count, rows, lanes = own.shape
    return pl.pallas_call(
        functools.partial(keys_kernel, count, heads, steps),
        out_shape=[
            jax.ShapeDtypeStruct((count * rows, lanes), own.dtype),
            jax.ShapeDtypeStruct((heads, lanes), jnp.float32),
        ],
        in_specs=[pl.BlockSpec(memory_space=pltpu.HBM)]
        + [pl.BlockSpec(memory_space=pltpu.VMEM)] * len(pieces)
        + [pl.BlockSpec(memory_space=pltpu.HBM)] * 2
        + [pl.BlockSpec(memory_space=pltpu.VMEM)],
        out_specs=[pl.BlockSpec(memory_space=pltpu.HBM), pl.BlockSpec(memory_space=pltpu.VMEM)],
        scratch_shapes=[
            pltpu.VMEM((rows, lanes), own.dtype),
            pltpu.VMEM((count, rows, lanes), jnp.float32),
            pltpu.VMEM((2, rows, lanes), jnp.float32),
            pltpu.VMEM((2, rows, lanes), jnp.float32),
            pltpu.VMEM((2, rows, lanes), own.dtype),
            pltpu.SemaphoreType.DMA,
            pltpu.SemaphoreType.DMA((2, 2)),
            pltpu.SemaphoreType.DMA((2,)),
        ],
        compiler_params=pltpu.CompilerParams(vmem_limit_bytes=24 << 20),
        cost_estimate=pl.CostEstimate(flops=count * rows * lanes * 200, bytes_accessed=count * rows * lanes * 8, transcendentals=0),
    )(in_hbm(own), *pieces, in_hbm(cosine), in_hbm(sine), gain)


def place_kernel(count, steps, own, *refs):
    number = len(steps)
    if own:
        local, refs = refs[1], refs[2:]
    else:
        refs = refs[1:]
    pieces, whole = refs[:number], refs[number]
    rows = whole.shape[0] // count
    me = lax.axis_index(GROUP)
    if own:
        block, in_sem, sems = refs[number + 1 :]
        first = pltpu.make_async_copy(local.at[me], block, in_sem)
        first.start()
    else:
        sems = refs[number + 1]
    copies = [
        pltpu.make_async_copy(piece, whole.at[pl.ds(sender(me, step, count) * rows, rows)], sems.at[slot])
        for slot, (step, piece) in enumerate(zip(steps, pieces))
    ]
    for copy in copies:
        copy.start()
    if own:
        first.wait()
        last = pltpu.make_async_copy(block, whole.at[pl.ds(me * rows, rows)], in_sem)
        last.start()
        last.wait()
    for copy in copies:
        copy.wait()


def place(before, own, pieces, steps, count):
    rows, lanes = pieces[0].shape
    number = len(steps)
    scratch = [pltpu.SemaphoreType.DMA((number,))]
    operands = [in_hbm(before)]
    if own is not None:
        operands.append(in_hbm(own))
        scratch = [pltpu.VMEM((rows, lanes), own.dtype), pltpu.SemaphoreType.DMA] + scratch
    return pl.pallas_call(
        functools.partial(place_kernel, count, steps, own is not None),
        out_shape=pltpu.HBM((count * rows, lanes), pieces[0].dtype),
        in_specs=[pl.BlockSpec(memory_space=pltpu.HBM)] * len(operands)
        + [pl.BlockSpec(memory_space=pltpu.VMEM)] * number,
        out_specs=pl.BlockSpec(memory_space=pltpu.HBM),
        scratch_shapes=scratch,
        input_output_aliases={} if own is not None else {0: 0},
        compiler_params=pltpu.CompilerParams(vmem_limit_bytes=4 << 20),
    )(*operands, *pieces)


def local(raw_keys, raw_values, turn_angle, key_gain):
    count, length, heads, lanes = raw_keys.shape
    rows = length * heads
    keys = raw_keys.reshape(count, rows, lanes)
    values = raw_values.reshape(count, rows, lanes)
    steps, value_steps = orders(count)
    early = cut(keys, steps[:1])
    early += cut(keys, steps[1:])
    late = cut(values, value_steps)
    key_pieces = exchange(early, steps, count)
    value_pieces = exchange(late, value_steps, count)
    cosine, sine = tables(turn_angle, heads)
    stored_keys, key_scale = finish_keys(keys, key_pieces, cosine, sine, key_gain.reshape(1, lanes), steps, heads)
    arrived = dict(zip(value_steps, value_pieces))
    stored_values, own = key_scale, values
    for group in (value_steps[:-3], value_steps[-3:-2], value_steps[-2:-1], value_steps[-1:]):
        if not group:
            continue
        stored_values = place(stored_values, own, [arrived[step] for step in group], group, count)
        own = None
    whole = (1, count * length, heads, lanes)
    return stored_keys.reshape(whole), stored_values.reshape(whole), key_scale[None]


def solution(mesh):
    in_specs = (
        P(None, GROUP, "model", None),
        P(None, GROUP, "model", None),
        P(),
        P(),
    )
    out_specs = (
        P(GROUP, None, "model", None),
        P(GROUP, None, "model", None),
        P(GROUP, "model", None),
    )
    return jax.shard_map(local, mesh=mesh, in_specs=in_specs, out_specs=out_specs, check_vma=False)
```

```python
import functools

import jax
import jax.numpy as jnp
from jax import lax
from jax.experimental import pallas as pl
from jax.experimental.pallas import tpu as pltpu
from jax.sharding import PartitionSpec as P


GROUP = ("farcp", "nearcp")
TILE = 128
UNROLL = 2
PARTS = 2


def partner(me, step, count):
    return me ^ step if count & (count - 1) == 0 else (me + step) % count


def sender(me, step, count):
    return me ^ step if count & (count - 1) == 0 else (me + count - step) % count


def orders(count):
    def hops(step):
        return bin(step >> 1).count("1")

    steps = range(1, count)
    keys = sorted(steps, key=lambda step: (step < 2, step & 1, -hops(step), step))
    values = sorted(steps, key=lambda step: (hops(step), step & 1, -step))
    return tuple(keys), tuple(values)


def in_hbm(array):
    return pltpu.with_memory_space_constraint(array, pltpu.HBM)


def cut_kernel(count, steps, whole, *refs):
    pieces, sems = refs[: len(steps)], refs[len(steps)]
    me = lax.axis_index(GROUP)
    copies = [
        pltpu.make_async_copy(whole.at[partner(me, step, count)], piece, sems.at[slot])
        for slot, (step, piece) in enumerate(zip(steps, pieces))
    ]
    for copy in copies:
        copy.start()
    for copy in copies:
        copy.wait()


def cut(whole, steps):
    count, rows, lanes = whole.shape
    return pl.pallas_call(
        functools.partial(cut_kernel, count, steps),
        out_shape=[pltpu.VMEM((rows, lanes), whole.dtype)] * len(steps),
        in_specs=[pl.BlockSpec(memory_space=pltpu.HBM)],
        out_specs=[pl.BlockSpec(memory_space=pltpu.VMEM)] * len(steps),
        scratch_shapes=[pltpu.SemaphoreType.DMA((len(steps),))],
        compiler_params=pltpu.CompilerParams(vmem_limit_bytes=8 << 20),
    )(in_hbm(whole))


def exchange(pieces, steps, count):
    moved = []
    for step, piece in zip(steps, pieces):
        pairs = [(source, int(partner(source, step, count))) for source in range(count)]
        moved.append(lax.ppermute(piece, GROUP, pairs))
    return moved


def table_kernel(heads, angle, cosine, sine):
    turn = angle[...]
    c, s = jnp.cos(turn), jnp.sin(turn)
    c = jnp.concatenate([c, c], axis=0).T
    s = jnp.concatenate([-s, s], axis=0).T
    for head in range(heads):
        at = pl.ds(head, c.shape[0], stride=heads)
        cosine[at, :] = c
        sine[at, :] = s


def tables(turn_angle, heads, block=512):
    length, half = turn_angle.shape
    shape = pltpu.HBM((length * heads, 2 * half), jnp.float32)
    return pl.pallas_call(
        functools.partial(table_kernel, heads),
        out_shape=[shape, shape],
        grid=(length // block,),
        in_specs=[pl.BlockSpec((half, block), lambda i: (0, i))],
        out_specs=[pl.BlockSpec((block * heads, 2 * half), lambda i: (i, 0))] * 2,
        compiler_params=pltpu.CompilerParams(vmem_limit_bytes=8 << 20),
        cost_estimate=pl.CostEstimate(flops=length * half * 400, bytes_accessed=length * half * 40, transcendentals=0),
    )(in_hbm(turn_angle.T))


def keys_kernel(count, heads, steps, own, *refs):
    number = len(steps)
    pieces = refs[:number]
    cosine, sine, gain, stored, scale = refs[number : number + 5]
    block, turned, cos_in, sin_in, out, in_sems, tab_sems, out_sems = refs[number + 5 :]
    rows, lanes = block.shape
    half = lanes // 2
    me = lax.axis_index(GROUP)
    sources = [me] + [sender(me, step, count) for step in steps]
    first = pltpu.make_async_copy(own.at[me], block, in_sems)
    first.start()

    def fetch(slot):
        part = pl.ds(sources[slot] * rows, rows)
        return (
            pltpu.make_async_copy(cosine.at[part], cos_in.at[slot % 2], tab_sems.at[slot % 2, 0]),
            pltpu.make_async_copy(sine.at[part], sin_in.at[slot % 2], tab_sems.at[slot % 2, 1]),
        )

    for copy in fetch(0):
        copy.start()
    first.wait()
    peak = jnp.zeros((8, lanes), jnp.float32)
    factor = gain[...]
    for slot in range(number + 1):
        piece = block if slot == 0 else pieces[slot - 1]
        for copy in fetch(slot):
            copy.wait()
        if slot < number:
            for copy in fetch(slot + 1):
                copy.start()

        def turn(index, peak, slot=slot, piece=piece):
            part = pl.ds(pl.multiple_of(index * TILE, TILE), TILE)
            wide = piece[part, :].astype(jnp.float32)
            mean = jnp.sum(wide * wide, axis=-1, keepdims=True) * (1.0 / lanes)
            wide = wide * lax.rsqrt(mean + 1e-06) * factor
            wide = wide * cos_in[slot % 2, part, :] + pltpu.roll(wide, half, 1) * sin_in[slot % 2, part, :]
            turned[slot, part, :] = wide
            return jnp.maximum(peak, jnp.max(jnp.abs(wide).reshape(TILE // 8, 8, lanes), axis=0))

        peak = lax.fori_loop(0, rows // TILE, turn, peak, unroll=UNROLL)
    tops = [peak[head : head + 1] for head in range(heads)]
    for row in range(heads, 8):
        tops[row % heads] = jnp.maximum(tops[row % heads], peak[row : row + 1])
    top = jnp.concatenate(tops, axis=0)
    scale[...] = top
    inverse = 1.0 / jnp.concatenate([top] * (8 // heads), axis=0)
    for slot in range(number + 1):
        copy = pltpu.make_async_copy(
            out.at[slot % 2], stored.at[pl.ds(sources[slot] * rows, rows)], out_sems.at[slot % 2]
        )
        if slot >= 2:
            copy.wait()

        def narrow(index, carry, slot=slot):
            part = pl.ds(pl.multiple_of(index * TILE, TILE), TILE)
            wide = turned[slot, part, :].reshape(TILE // 8, 8, lanes) * inverse[None]
            out[slot % 2, part, :] = wide.reshape(TILE, lanes).astype(out.dtype)
            return carry

        lax.fori_loop(0, rows // TILE, narrow, 0, unroll=UNROLL)
        copy.start()
    for slot in range(max(number - 1, 0), number + 1):
        pltpu.make_async_copy(
            out.at[slot % 2], stored.at[pl.ds(sources[slot] * rows, rows)], out_sems.at[slot % 2]
        ).wait()


def finish_keys(own, pieces, cosine, sine, gain, steps, heads):
    count, rows, lanes = own.shape
    return pl.pallas_call(
        functools.partial(keys_kernel, count, heads, steps),
        out_shape=[
            jax.ShapeDtypeStruct((count * rows, lanes), own.dtype),
            jax.ShapeDtypeStruct((heads, lanes), jnp.float32),
        ],
        in_specs=[pl.BlockSpec(memory_space=pltpu.HBM)]
        + [pl.BlockSpec(memory_space=pltpu.VMEM)] * len(pieces)
        + [pl.BlockSpec(memory_space=pltpu.HBM)] * 2
        + [pl.BlockSpec(memory_space=pltpu.VMEM)],
        out_specs=[pl.BlockSpec(memory_space=pltpu.HBM), pl.BlockSpec(memory_space=pltpu.VMEM)],
        scratch_shapes=[
            pltpu.VMEM((rows, lanes), own.dtype),
            pltpu.VMEM((count, rows, lanes), jnp.float32),
            pltpu.VMEM((2, rows, lanes), jnp.float32),
            pltpu.VMEM((2, rows, lanes), jnp.float32),
            pltpu.VMEM((2, rows, lanes), own.dtype),
            pltpu.SemaphoreType.DMA,
            pltpu.SemaphoreType.DMA((2, 2)),
            pltpu.SemaphoreType.DMA((2,)),
        ],
        compiler_params=pltpu.CompilerParams(vmem_limit_bytes=24 << 20),
        cost_estimate=pl.CostEstimate(flops=count * rows * lanes * 200, bytes_accessed=count * rows * lanes * 8, transcendentals=0),
    )(in_hbm(own), *pieces, in_hbm(cosine), in_hbm(sine), gain)


def place_kernel(count, steps, own, *refs):
    number = len(steps)
    if own:
        local, refs = refs[1], refs[2:]
    else:
        refs = refs[1:]
    pieces, whole = refs[:number], refs[number]
    rows = whole.shape[0] // count
    me = lax.axis_index(GROUP)
    if own:
        block, in_sem, sems = refs[number + 1 :]
        first = pltpu.make_async_copy(local.at[me], block, in_sem)
        first.start()
    else:
        sems = refs[number + 1]
    size = rows // PARTS
    copies = [
        pltpu.make_async_copy(
            piece.at[pl.ds(part * size, size)],
            whole.at[pl.ds(sender(me, step, count) * rows + part * size, size)],
            sems.at[slot, part],
        )
        for slot, (step, piece) in enumerate(zip(steps, pieces))
        for part in range(PARTS)
    ]
    for copy in copies:
        copy.start()
    if own:
        first.wait()
        last = pltpu.make_async_copy(block, whole.at[pl.ds(me * rows, rows)], in_sem)
        last.start()
        last.wait()
    for copy in copies:
        copy.wait()


def place(before, own, pieces, steps, count):
    rows, lanes = pieces[0].shape
    number = len(steps)
    scratch = [pltpu.SemaphoreType.DMA((number, PARTS))]
    operands = [in_hbm(before)]
    if own is not None:
        operands.append(in_hbm(own))
        scratch = [pltpu.VMEM((rows, lanes), own.dtype), pltpu.SemaphoreType.DMA] + scratch
    return pl.pallas_call(
        functools.partial(place_kernel, count, steps, own is not None),
        out_shape=pltpu.HBM((count * rows, lanes), pieces[0].dtype),
        in_specs=[pl.BlockSpec(memory_space=pltpu.HBM)] * len(operands)
        + [pl.BlockSpec(memory_space=pltpu.VMEM)] * number,
        out_specs=pl.BlockSpec(memory_space=pltpu.HBM),
        scratch_shapes=scratch,
        input_output_aliases={} if own is not None else {0: 0},
        compiler_params=pltpu.CompilerParams(vmem_limit_bytes=4 << 20),
    )(*operands, *pieces)


def local(raw_keys, raw_values, turn_angle, key_gain):
    count, length, heads, lanes = raw_keys.shape
    rows = length * heads
    keys = raw_keys.reshape(count, rows, lanes)
    values = raw_values.reshape(count, rows, lanes)
    steps, value_steps = orders(count)
    early = cut(keys, steps[:1])
    early += cut(keys, steps[1:])
    late = cut(values, value_steps)
    key_pieces = exchange(early, steps, count)
    value_pieces = exchange(late, value_steps, count)
    cosine, sine = tables(turn_angle, heads)
    stored_keys, key_scale = finish_keys(keys, key_pieces, cosine, sine, key_gain.reshape(1, lanes), steps, heads)
    arrived = dict(zip(value_steps, value_pieces))
    stored_values, own = key_scale, values
    for group in (value_steps[:-3], value_steps[-3:-2], value_steps[-2:-1], value_steps[-1:]):
        if not group:
            continue
        stored_values = place(stored_values, own, [arrived[step] for step in group], group, count)
        own = None
    whole = (1, count * length, heads, lanes)
    return stored_keys.reshape(whole), stored_values.reshape(whole), key_scale[None]


def solution(mesh):
    in_specs = (
        P(None, GROUP, "model", None),
        P(None, GROUP, "model", None),
        P(),
        P(),
    )
    out_specs = (
        P(GROUP, None, "model", None),
        P(GROUP, None, "model", None),
        P(GROUP, "model", None),
    )
    return jax.shard_map(local, mesh=mesh, in_specs=in_specs, out_specs=out_specs, check_vma=False)
```

```python
import functools

import jax
import jax.numpy as jnp
from jax import lax
from jax.experimental import pallas as pl
from jax.experimental.pallas import tpu as pltpu
from jax.sharding import PartitionSpec as P


GROUP = ("farcp", "nearcp")
TILE = 128
UNROLL = 2
PARTS = 2


def partner(me, step, count):
    return me ^ step if count & (count - 1) == 0 else (me + step) % count


def sender(me, step, count):
    return me ^ step if count & (count - 1) == 0 else (me + count - step) % count


def orders(count):
    def hops(step):
        return bin(step >> 1).count("1")

    steps = range(1, count)
    keys = sorted(steps, key=lambda step: (step < 2, step & 1, -hops(step), step))
    values = sorted(steps, key=lambda step: (hops(step), step & 1, -step))
    return tuple(keys), tuple(values)


def in_hbm(array):
    return pltpu.with_memory_space_constraint(array, pltpu.HBM)


def cut_kernel(count, steps, whole, *refs):
    pieces, sems = refs[: len(steps)], refs[len(steps)]
    me = lax.axis_index(GROUP)
    copies = [
        pltpu.make_async_copy(whole.at[partner(me, step, count)], piece, sems.at[slot])
        for slot, (step, piece) in enumerate(zip(steps, pieces))
    ]
    for copy in copies:
        copy.start()
    for copy in copies:
        copy.wait()


def cut(whole, steps):
    count, rows, lanes = whole.shape
    return pl.pallas_call(
        functools.partial(cut_kernel, count, steps),
        out_shape=[pltpu.VMEM((rows, lanes), whole.dtype)] * len(steps),
        in_specs=[pl.BlockSpec(memory_space=pltpu.HBM)],
        out_specs=[pl.BlockSpec(memory_space=pltpu.VMEM)] * len(steps),
        scratch_shapes=[pltpu.SemaphoreType.DMA((len(steps),))],
        compiler_params=pltpu.CompilerParams(vmem_limit_bytes=8 << 20),
    )(in_hbm(whole))


def exchange(pieces, steps, count):
    moved = []
    for step, piece in zip(steps, pieces):
        pairs = [(source, int(partner(source, step, count))) for source in range(count)]
        moved.append(lax.ppermute(piece, GROUP, pairs))
    return moved


def table_kernel(heads, angle, cosine, sine):
    turn = angle[...]
    c, s = jnp.cos(turn), jnp.sin(turn)
    c = jnp.concatenate([c, c], axis=0).T
    s = jnp.concatenate([-s, s], axis=0).T
    for head in range(heads):
        at = pl.ds(head, c.shape[0], stride=heads)
        cosine[at, :] = c
        sine[at, :] = s


def tables(turn_angle, heads, block=512):
    length, half = turn_angle.shape
    shape = pltpu.VMEM((length * heads, 2 * half), jnp.float32)
    return pl.pallas_call(
        functools.partial(table_kernel, heads),
        out_shape=[shape, shape],
        grid=(length // block,),
        in_specs=[pl.BlockSpec((half, block), lambda i: (0, i))],
        out_specs=[pl.BlockSpec((block * heads, 2 * half), lambda i: (i, 0))] * 2,
        compiler_params=pltpu.CompilerParams(vmem_limit_bytes=8 << 20),
        cost_estimate=pl.CostEstimate(flops=length * half * 400, bytes_accessed=length * half * 40, transcendentals=0),
    )(in_hbm(turn_angle.T))


def keys_kernel(count, heads, steps, *refs):
    number = len(steps)
    pieces = refs[:number]
    cosine, sine, gain, stored, scale, turned, out, out_sems = refs[number:]
    rows, lanes = pieces[0].shape
    half = lanes // 2
    me = lax.axis_index(GROUP)
    starts = [pl.multiple_of(sender(me, step, count) * rows, rows) for step in steps]
    peak = jnp.zeros((8, lanes), jnp.float32)
    factor = gain[...]
    for slot, piece in enumerate(pieces):

        def turn(index, peak, slot=slot, piece=piece):
            part = pl.ds(pl.multiple_of(index * TILE, TILE), TILE)
            place = pl.ds(pl.multiple_of(starts[slot] + index * TILE, TILE), TILE)
            wide = piece[part, :].astype(jnp.float32)
            mean = jnp.sum(wide * wide, axis=-1, keepdims=True) * (1.0 / lanes)
            wide = wide * lax.rsqrt(mean + 1e-06) * factor
            wide = wide * cosine[place, :] + pltpu.roll(wide, half, 1) * sine[place, :]
            turned[slot, part, :] = wide
            return jnp.maximum(peak, jnp.max(jnp.abs(wide).reshape(TILE // 8, 8, lanes), axis=0))

        peak = lax.fori_loop(0, rows // TILE, turn, peak, unroll=UNROLL)
    tops = [peak[head : head + 1] for head in range(heads)]
    for row in range(heads, 8):
        tops[row % heads] = jnp.maximum(tops[row % heads], peak[row : row + 1])
    top = jnp.concatenate(tops, axis=0)
    scale[...] = top
    inverse = 1.0 / jnp.concatenate([top] * (8 // heads), axis=0)
    copies = [
        pltpu.make_async_copy(out.at[slot % 2], stored.at[pl.ds(starts[slot], rows)], out_sems.at[slot % 2])
        for slot in range(number)
    ]
    for slot in range(number):
        if slot >= 2:
            copies[slot - 2].wait()

        def narrow(index, carry, slot=slot):
            part = pl.ds(pl.multiple_of(index * TILE, TILE), TILE)
            wide = turned[slot, part, :].reshape(TILE // 8, 8, lanes) * inverse[None]
            out[slot % 2, part, :] = wide.reshape(TILE, lanes).astype(out.dtype)
            return carry

        lax.fori_loop(0, rows // TILE, narrow, 0, unroll=UNROLL)
        copies[slot].start()
    for copy in copies[-2:]:
        copy.wait()


def finish_keys(pieces, cosine, sine, gain, steps, heads):
    count = len(steps)
    rows, lanes = pieces[0].shape
    dtype = pieces[0].dtype
    return pl.pallas_call(
        functools.partial(keys_kernel, count, heads, steps),
        out_shape=[
            pltpu.HBM((count * rows, lanes), dtype),
            jax.ShapeDtypeStruct((heads, lanes), jnp.float32),
        ],
        in_specs=[pl.BlockSpec(memory_space=pltpu.VMEM)] * (len(pieces) + 3),
        out_specs=[pl.BlockSpec(memory_space=pltpu.HBM), pl.BlockSpec(memory_space=pltpu.VMEM)],
        scratch_shapes=[
            pltpu.VMEM((count, rows, lanes), jnp.float32),
            pltpu.VMEM((2, rows, lanes), dtype),
            pltpu.SemaphoreType.DMA((2,)),
        ],
        compiler_params=pltpu.CompilerParams(vmem_limit_bytes=16 << 20),
        cost_estimate=pl.CostEstimate(flops=count * rows * lanes * 200, bytes_accessed=count * rows * lanes * 8, transcendentals=0),
    )(*pieces, cosine, sine, gain)


def place_kernel(count, steps, before, *refs):
    del before
    number = len(steps)
    pieces, whole, sems = refs[:number], refs[number], refs[number + 1]
    rows = whole.shape[0] // count
    me = lax.axis_index(GROUP)
    size = rows // PARTS
    copies = [
        pltpu.make_async_copy(
            piece.at[pl.ds(part * size, size)],
            whole.at[pl.ds(sender(me, step, count) * rows + part * size, size)],
            sems.at[slot, part],
        )
        for slot, (step, piece) in enumerate(zip(steps, pieces))
        for part in range(PARTS)
    ]
    for copy in copies:
        copy.start()
    for copy in copies:
        copy.wait()


def place(before, pieces, steps, count):
    rows, lanes = pieces[0].shape
    number = len(steps)
    whole = pltpu.HBM((count * rows, lanes), pieces[0].dtype)
    return pl.pallas_call(
        functools.partial(place_kernel, count, steps),
        out_shape=whole,
        in_specs=[pl.BlockSpec(memory_space=pltpu.HBM)] + [pl.BlockSpec(memory_space=pltpu.VMEM)] * number,
        out_specs=pl.BlockSpec(memory_space=pltpu.HBM),
        scratch_shapes=[pltpu.SemaphoreType.DMA((number, PARTS))],
        input_output_aliases={0: 0} if before.shape == whole.shape else {},
        compiler_params=pltpu.CompilerParams(vmem_limit_bytes=4 << 20),
    )(in_hbm(before), *pieces)


def local(raw_keys, raw_values, turn_angle, key_gain):
    count, length, heads, lanes = raw_keys.shape
    rows = length * heads
    keys = raw_keys.reshape(count, rows, lanes)
    values = raw_values.reshape(count, rows, lanes)
    steps, value_steps = orders(count)
    early = cut(keys, steps[:1])
    early = [*early, *cut(keys, steps[1:] + (0,))]
    late = cut(values, value_steps + (0,))
    key_pieces = exchange(early[:-1], steps, count) + [early[-1]]
    value_pieces = exchange(late[:-1], value_steps, count)
    cosine, sine = tables(turn_angle, heads)
    stored_keys, key_scale = finish_keys(key_pieces, cosine, sine, key_gain.reshape(1, lanes), steps + (0,), heads)
    arrived = {0: late[-1], **dict(zip(value_steps, value_pieces))}
    stored_values = key_scale
    for group in ((0,) + value_steps[:-3], value_steps[-3:-2], value_steps[-2:-1], value_steps[-1:]):
        if group:
            stored_values = place(stored_values, [arrived[step] for step in group], group, count)
    whole = (1, count * length, heads, lanes)
    return stored_keys.reshape(whole), stored_values.reshape(whole), key_scale[None]


def solution(mesh):
    in_specs = (
        P(None, GROUP, "model", None),
        P(None, GROUP, "model", None),
        P(),
        P(),
    )
    out_specs = (
        P(GROUP, None, "model", None),
        P(GROUP, None, "model", None),
        P(GROUP, "model", None),
    )
    return jax.shard_map(local, mesh=mesh, in_specs=in_specs, out_specs=out_specs, check_vma=False)
```
